32 devices in a mesh: seq: 8 (over z, core), head: 4 (over y, x).
Axes of the slice: x: 2, y: 2, z: 4, core: 2. Of those that a mesh axis runs over, the one named last changes fastest.
Arguments:
- queries: bfloat16 [4096, 8192], P('seq', 'head'), may hold values from -18 to 18
- key_rows: bfloat16 [4096, 8192], P('seq', 'head'), may hold values from -6 to 6
- values: bfloat16 [4096, 8192], P('seq', 'head'), may hold values from -6 to 6
- norm_gain: float32 [8192], P('head'), may hold values from 0.25 to 1.75
- cotangent: bfloat16 [4096, 8192], P('seq', 'head'), may hold values from -6 to 6
Outputs:
- normed: bfloat16 [4096, 8192], P('seq', 'head')
- query_grad: bfloat16 [4096, 8192], P('seq', 'head')
- key_grad: bfloat16 [4096, 8192], P('seq', 'head')
- value_grad: bfloat16 [4096, 8192], P('seq', 'head')
The draws below stay inside these ranges and needn't reach their ends.
All inputs are finite; a program needn't handle non-finite values.
Results may differ from the reference program's by a relative error of at most 0.0051.
Values sent between devices are 32-bit elements; how exact they have to be, the bound alone decides.
No kernel may reach another device: no remote copies, remote signals or barrier semaphores. Data moves between devices by JAX's collectives and lax.ppermute only.
A program may use at most 128 MiB of HBM per device.

```python
import jax
import jax.numpy as jnp
from jax import lax

HEADS = 64
HEAD_DIM = 128
TOK_DEV = 512
WIDTH = 8192
TOKENS = 4096
N_SEQ = 8


def draw_queries(key, part):
    position = jnp.arange(HEADS, dtype=jnp.float32) / max(HEADS - 1, 1)
    base = jnp.clip(jax.random.normal(key, (TOKENS, HEADS, HEAD_DIM), jnp.float32), -4.0, 4.0)
    scale = 3.0 ** position
    return (base * scale[None, :, None]).reshape(TOKENS, HEADS * HEAD_DIM).astype(jnp.bfloat16)


def block_levels(rng, dims, pieces, low, largest):
    factor_of = 1.0
    for dim, shards_of in pieces:
        steps = jax.random.uniform(jax.random.fold_in(jax.random.fold_in(rng, 6), dim), (shards_of,), jnp.float32, low / len(pieces), largest / len(pieces))
        factor_of = factor_of * jnp.repeat(jnp.exp(steps), dims[dim] // shards_of).reshape((-1,) + (1,) * (len(dims) - 1 - dim))
    return factor_of


def noise(key, shape, spread, limit, split=(), kind=jnp.bfloat16):
    drawn = jax.random.normal(key, shape, jnp.float32) * spread
    if len(split) > 0:
        drawn = block_levels(key, shape, split, -0.22, 0.18) * drawn
    return jnp.clip(drawn, min=-limit, max=limit).astype(kind)


def setup_inputs(seed: int = 0) -> dict:
    key_list = jax.random.split(jax.random.key(seed), 6)
    queries = draw_queries(jax.random.fold_in(key_list[5], 71), 0)
    key_rows = noise(key_list[1], (TOKENS, WIDTH), 1.0, 6.0, ((0, 8), (1, 4)))
    values = noise(key_list[2], (TOKENS, WIDTH), 1.0, 6.0, ((0, 8), (1, 4)))
    norm_gain = jnp.clip(1.0 + 0.15 * jax.random.normal(key_list[3], (WIDTH,), jnp.float32), 0.25, 1.75)
    cotangent = noise(key_list[4], (TOKENS, WIDTH), 1.0, 6.0, ((0, 8), (1, 4)))
    return {"queries": queries, "key_rows": key_rows, "values": values, "norm_gain": norm_gain, "cotangent": cotangent}


epsilon = 1e-06
highest = lax.Precision.HIGHEST

def lower_mask(count):
    rows = lax.broadcasted_iota(jnp.int32, (count, count), 0)
    cols = lax.broadcasted_iota(jnp.int32, (count, count), 1)
    return cols <= rows

def block_output(query_part, key_part, value_part, prefix):
    qf = query_part.astype(jnp.float32)
    inter = jnp.einsum('thi,hij->thj', qf, prefix, precision=highest)
    scores = jnp.einsum('thi,shi->hts', qf, key_part.astype(jnp.float32), precision=highest)
    weights = jnp.where(lower_mask(query_part.shape[0])[None], scores, 0.0).astype(jnp.bfloat16)
    intra = jnp.einsum('hts,shj->thj', weights.astype(jnp.float32), value_part.astype(jnp.float32), precision=highest)
    return (inter + intra, weights)

def reference(queries, key_rows, values, norm_gain, cotangent):
    blocks = N_SEQ
    shape = (blocks, TOK_DEV, HEADS, HEAD_DIM)
    query_parts = queries.reshape(shape)
    key_parts = key_rows.reshape(shape)
    value_parts = values.reshape(shape)
    grad_parts = cotangent.reshape(shape)
    width = HEADS * HEAD_DIM

    def forward_step(state, inputs):
        query_part, key_part, value_part = inputs
        raw, weights = block_output(query_part, key_part, value_part, state)
        flat = raw.reshape(TOK_DEV, width)
        rms = jnp.sqrt(lax.optimization_barrier(jnp.sum(flat * flat, axis=1)) / width + epsilon)
        normed = (norm_gain[None, :] * flat / rms[:, None]).astype(jnp.bfloat16)
        local = jnp.einsum('thi,thj->hij', key_part.astype(jnp.float32), value_part.astype(jnp.float32), precision=highest)
        return (state + local, (normed, state))
    start = jnp.zeros((HEADS, HEAD_DIM, HEAD_DIM), jnp.float32)
    final, (normed, prefixes) = lax.scan(forward_step, start, (query_parts, key_parts, value_parts))

    def backward_step(suffix, inputs):
        query_part, key_part, value_part, grad_part, prefix = inputs
        raw, weights = block_output(query_part, key_part, value_part, prefix)
        flat = raw.reshape(TOK_DEV, width)
        rms = jnp.sqrt(lax.optimization_barrier(jnp.sum(flat * flat, axis=1)) / width + epsilon)
        scaled = norm_gain[None, :] * grad_part.reshape(TOK_DEV, width).astype(jnp.float32)
        dot = lax.optimization_barrier(jnp.sum(scaled * flat, axis=1))
        raw_grad = (scaled / rms[:, None] - flat * (dot / (width * rms ** 3))[:, None]).astype(jnp.bfloat16)
        raw_grad = raw_grad.reshape(TOK_DEV, HEADS, HEAD_DIM)
        gf = raw_grad.astype(jnp.float32)
        qf = query_part.astype(jnp.float32)
        kf = key_part.astype(jnp.float32)
        vf = value_part.astype(jnp.float32)
        grad_scores = jnp.einsum('thj,shj->hts', gf, vf, precision=highest)
        grad_weights = jnp.where(lower_mask(TOK_DEV)[None], grad_scores, 0.0).astype(jnp.bfloat16).astype(jnp.float32)
        query_grad = jnp.einsum('thj,hij->thi', gf, prefix, precision=highest) + jnp.einsum('hts,shi->thi', grad_weights, kf, precision=highest)
        key_grad = jnp.einsum('shj,hij->shi', vf, suffix, precision=highest) + jnp.einsum('hts,thi->shi', grad_weights, qf, precision=highest)
        value_grad = jnp.einsum('shi,hij->shj', kf, suffix, precision=highest) + jnp.einsum('hts,thj->shj', weights.astype(jnp.float32), gf, precision=highest)
        local = jnp.einsum('thi,thj->hij', qf, gf, precision=highest)
        return (suffix + local, (query_grad.astype(jnp.bfloat16), key_grad.astype(jnp.bfloat16), value_grad.astype(jnp.bfloat16)))
    last, (query_grad, key_grad, value_grad) = lax.scan(backward_step, start, (query_parts, key_parts, value_parts, grad_parts, prefixes), reverse=True)
    full = (TOKENS, width)
    return (normed.reshape(full), query_grad.reshape(full), key_grad.reshape(full), value_grad.reshape(full))
```

```python
import functools

import jax
import jax.numpy as jnp
from jax import lax
from jax.experimental import pallas as pl
from jax.experimental.pallas import tpu as pltpu
from jax.sharding import PartitionSpec as P

HEAD_DIM = 128
TILE = 256
CHUNKS = 4
epsilon = 1e-06


f32 = jnp.float32
bf16 = jnp.bfloat16


def dot_nn(a, b):
    return lax.dot_general(a, b, (((1,), (0,)), ((), ())), preferred_element_type=f32)


def dot_nt(a, b):
    return lax.dot_general(a, b, (((1,), (1,)), ((), ())), preferred_element_type=f32)


def dot_tn(a, b):
    return lax.dot_general(a, b, (((0,), (0,)), ((), ())), preferred_element_type=f32)


def split(x, axis):
    high = x.astype(bf16)
    low = (x - high.astype(f32)).astype(bf16)
    return jnp.concatenate([high, low], axis=axis)


def twice(x):
    return jnp.concatenate([x, x], axis=1)


def cols(h):
    return pl.ds(h * HEAD_DIM, HEAD_DIM)


def diag_mask(size, upper):
    rows = lax.broadcasted_iota(jnp.int32, (size, size), 0)
    columns = lax.broadcasted_iota(jnp.int32, (size, size), 1)
    return columns >= rows if upper else columns <= rows


def lower_products(left, right, tile, i):
    rows = left[i * tile : (i + 1) * tile]
    scores = dot_nt(rows, right[: (i + 1) * tile])
    diag = jnp.where(diag_mask(tile, False), scores[:, i * tile :], 0.0)
    if i == 0:
        return diag.astype(bf16)
    return jnp.concatenate([scores[:, : i * tile].astype(bf16), diag.astype(bf16)], axis=1)


def upper_products(left, right, tile, j):
    rows = left[j * tile : (j + 1) * tile]
    scores = dot_nt(rows, right[j * tile :])
    diag = jnp.where(diag_mask(tile, True), scores[:, :tile], 0.0)
    if (j + 1) * tile == left.shape[0]:
        return diag.astype(bf16)
    return jnp.concatenate([diag.astype(bf16), scores[:, tile:].astype(bf16)], axis=1)


def state_kernel(half, core_ref, key_ref, value_ref, mine_ref, send_ref):
    j = pl.program_id(0)
    for out, step in ((mine_ref, 0), (send_ref, 1)):

        @pl.when(j == step)
        def _(out=out):
            for h in range(half):
                out[h] = dot_tn(key_ref[:, cols(h)], value_ref[:, cols(h)])


def intra_kernel(heads, tile, q_ref, k_ref, v_ref, out_ref):
    for h in range(heads):
        q, k, v = q_ref[:, cols(h)], k_ref[:, cols(h)], v_ref[:, cols(h)]
        for i in range(q.shape[0] // tile):
            weights = lower_products(q, k, tile, i)
            out_ref[i * tile : (i + 1) * tile, cols(h)] = dot_nn(weights, v[: (i + 1) * tile])


def raw_kernel(half, core_ref, q_ref, intra_ref, grad_ref, gain_ref, own_ref, other_ref, sums_ref, raw_ref, out_ref, squares, products):
    j = pl.program_id(0)

    @pl.when(j == 0)
    def _():
        squares[...] = jnp.zeros_like(squares)
        products[...] = jnp.zeros_like(products)

    def body(state_ref):
        square = squares[...]
        product = products[...]
        for h in range(half):
            q = q_ref[:, cols(h)]
            raw = dot_nn(twice(q), split(state_ref[h], 0)) + intra_ref[:, cols(h)]
            raw_ref[:, cols(h)] = raw
            square = square + raw * raw
            product = product + (gain_ref[:, cols(h)] * grad_ref[:, cols(h)].astype(f32)) * raw
        squares[...] = square
        products[...] = product

    @pl.when(j == 0)
    def _():
        body(own_ref)

    @pl.when(j == 1)
    def _():
        body(other_ref)
        out_ref[0:1] = sums_ref[0:1] + jnp.sum(squares[...].T, axis=0, keepdims=True)
        out_ref[1:2] = sums_ref[1:2] + jnp.sum(products[...].T, axis=0, keepdims=True)


def scales_of(width, sums):
    rms = jnp.sqrt(sums[0:1] / width + epsilon)
    inverse = 1.0 / rms
    factor = sums[1:2] / (width * (rms * rms * rms))
    tokens = rms.shape[1]
    inverse = jnp.broadcast_to(inverse, (HEAD_DIM, tokens)).T
    factor = jnp.broadcast_to(factor, (HEAD_DIM, tokens)).T
    return inverse, factor


def grad_kernel(half, width, parts, core_ref, q_ref, raw_ref, grad_ref, gain_ref, *rest):
    sums_refs, (out_ref, mine_ref, send_ref, inverse_ref, factor_ref) = rest[:parts], rest[parts:]
    j = pl.program_id(0)

    @pl.when(j == 0)
    def _():
        total = sums_refs[0][...]
        for other in sums_refs[1:]:
            total = total + other[...]
        inverse, factor = scales_of(width, total)
        inverse_ref[...] = inverse
        factor_ref[...] = factor

    for out, step in ((mine_ref, 0), (send_ref, 1)):

        @pl.when(j == step)
        def _(out=out):
            for h in range(half):
                scaled = gain_ref[:, cols(h)] * grad_ref[:, cols(h)].astype(f32)
                raw_grad = scaled * inverse_ref[...] - raw_ref[:, cols(h)] * factor_ref[...]
                raw_grad = raw_grad.astype(bf16)
                out_ref[:, cols(h)] = raw_grad
                out[h] = dot_tn(q_ref[:, cols(h)], raw_grad)


def local_kernel(half, tile, core_ref, q_ref, k_ref, v_ref, raw_ref, gain_ref, inverse_ref, rg_ref, own_ref, other_ref, normed_ref, dq_ref, dk_ref, dv_ref):
    j = pl.program_id(0)

    def body(state_ref):
        for h in range(half):
            q, k, v, rg = q_ref[:, cols(h)], k_ref[:, cols(h)], v_ref[:, cols(h)], rg_ref[:, cols(h)]
            normed_ref[:, cols(h)] = (gain_ref[:, cols(h)] * raw_ref[:, cols(h)] * inverse_ref[...]).astype(bf16)
            state = split(state_ref[h], 1)
            count = q.shape[0] // tile
            for i in range(count):
                rows = slice(i * tile, (i + 1) * tile)
                weights = lower_products(rg, v, tile, i)
                dq = dot_nn(weights, k[: (i + 1) * tile]) + dot_nt(twice(rg[rows]), state)
                dq_ref[rows, cols(h)] = dq.astype(bf16)
                dk_ref[rows, cols(h)] = dot_nn(upper_products(v, rg, tile, i), q[i * tile :])
                dv_ref[rows, cols(h)] = dot_nn(upper_products(k, q, tile, i), rg[i * tile :])

    @pl.when(j == 0)
    def _():
        body(own_ref)

    @pl.when(j == 1)
    def _():
        body(other_ref)


def final_kernel(half, core_ref, k_ref, v_ref, dkp_ref, dvp_ref, own_ref, other_ref, dk_ref, dv_ref):
    j = pl.program_id(0)

    def body(state_ref):
        for h in range(half):
            state = state_ref[h]
            dk = dkp_ref[:, cols(h)] + dot_nt(twice(v_ref[:, cols(h)]), split(state, 1))
            dv = dvp_ref[:, cols(h)] + dot_nn(twice(k_ref[:, cols(h)]), split(state, 0))
            dk_ref[:, cols(h)] = dk.astype(bf16)
            dv_ref[:, cols(h)] = dv.astype(bf16)

    @pl.when(j == 0)
    def _():
        body(own_ref)

    @pl.when(j == 1)
    def _():
        body(other_ref)


class Calls:
    def __init__(self, tokens, heads, chunks, core, width):
        self.tokens, self.heads, self.chunks, self.core, self.width = tokens, heads, chunks, core, width
        self.per_chunk = heads // chunks
        self.half = self.per_chunk // 2
        self.tile = min(TILE, tokens)

    def spec(self, k, rows=None):
        rows = self.tokens if rows is None else rows
        return pl.BlockSpec((rows, self.half * HEAD_DIM), lambda j, core: (0, 2 * k + (j + core[0]) % 2))

    def whole(self, shape):
        return pl.BlockSpec(shape, lambda j, core: (0,) * len(shape))

    def call(self, kernel, name, in_specs, out_specs, out_shape, args, scratch=(), flops=1):
        grid_spec = pltpu.PrefetchScalarGridSpec(
            num_scalar_prefetch=1, grid=(2,), in_specs=in_specs, out_specs=out_specs, scratch_shapes=scratch
        )
        return pl.pallas_call(
            kernel,
            grid_spec=grid_spec,
            out_shape=out_shape,
            name=name,
            compiler_params=pltpu.CompilerParams(
                dimension_semantics=("arbitrary",), vmem_limit_bytes=24 * 1024 * 1024
            ),
            cost_estimate=pl.CostEstimate(flops=int(flops), transcendentals=0, bytes_accessed=1024),
        )(self.core, *args)

    def state_shape(self):
        return (self.half, HEAD_DIM, HEAD_DIM)

    def chunk_shape(self, dtype):
        return jax.ShapeDtypeStruct((self.tokens, self.per_chunk * HEAD_DIM), dtype)

    def states(self, k, key, value):
        shape = jax.ShapeDtypeStruct(self.state_shape(), f32)
        return self.call(
            functools.partial(state_kernel, self.half), "state",
            [self.spec(k), self.spec(k)], [self.whole(self.state_shape())] * 2, [shape, shape], (key, value),
        )

    def intra(self, k, q, key, value):
        spec = self.spec(k)
        return self.call(
            lambda core, *refs: intra_kernel(self.half, self.tile, *refs), "intra",
            [spec] * 3, self.spec(0), self.chunk_shape(f32), (q, key, value), flops=2e9,
        )

    def raw(self, k, q, intra, grad, gain, own, other, sums):
        state = self.whole(self.state_shape())
        small = self.whole((2, self.tokens))
        return self.call(
            functools.partial(raw_kernel, self.half), "raw",
            [self.spec(k), self.spec(0), self.spec(k), self.spec(k, 1), state, state, small],
            [self.spec(0), small],
            [self.chunk_shape(f32), jax.ShapeDtypeStruct((2, self.tokens), f32)],
            (q, intra, grad, gain, own, other, sums),
            scratch=[pltpu.VMEM((self.tokens, HEAD_DIM), f32)] * 2,
        )

    def grads(self, k, q, raw, grad, gain, sums):
        shape = jax.ShapeDtypeStruct(self.state_shape(), f32)
        state = self.whole(self.state_shape())
        small = self.whole((2, self.tokens))
        wide = self.whole((self.tokens, HEAD_DIM))
        wide_shape = jax.ShapeDtypeStruct((self.tokens, HEAD_DIM), f32)
        return self.call(
            functools.partial(grad_kernel, self.half, self.width, len(sums)), "grads",
            [self.spec(k), self.spec(0), self.spec(k), self.spec(k, 1)] + [small] * len(sums),
            [self.spec(0), state, state, wide, wide],
            [self.chunk_shape(bf16), shape, shape, wide_shape, wide_shape],
            (q, raw, grad, gain, *sums),
        )

    def local(self, k, q, key, value, raw, gain, inverse, raw_grad, own, other):
        state = self.whole(self.state_shape())
        wide = self.whole((self.tokens, HEAD_DIM))
        spec = self.spec(k)
        return self.call(
            functools.partial(local_kernel, self.half, self.tile), "local",
            [spec, spec, spec, self.spec(0), self.spec(k, 1), wide, self.spec(0), state, state],
            [self.spec(0)] * 4,
            [self.chunk_shape(bf16), self.chunk_shape(bf16), self.chunk_shape(f32), self.chunk_shape(f32)],
            (q, key, value, raw, gain, inverse, raw_grad, own, other), flops=4e9,
        )

    def final(self, k, key, value, dkp, dvp, own, other):
        state = self.whole(self.state_shape())
        spec = self.spec(k)
        return self.call(
            functools.partial(final_kernel, self.half), "final",
            [spec, spec, self.spec(0), self.spec(0), state, state],
            [self.spec(0)] * 2, [self.chunk_shape(bf16)] * 2, (key, value, dkp, dvp, own, other),
        )


def swap(x, axis, pairs):
    return lax.ppermute(x, axis, [(a, b) for a, b in pairs] + [(b, a) for a, b in pairs])


def scan_chain(mine, send, forward):
    count = lax.axis_size("seq")
    index = lax.axis_index("seq")
    group, core = index // 2, index % 2
    groups = count // 2
    first = core == (1 if forward else 0)
    chunks = len(mine)
    partner = [swap(send[k], "seq", [(2 * g, 2 * g + 1) for g in range(groups)]) for k in range(chunks)]
    total = [mine[k] + partner[k] for k in range(chunks)]
    before = [jnp.zeros_like(total[k]) for k in range(chunks)]
    carried = list(total)
    for hop in range(1, groups):
        source, target = (hop - 1, hop) if forward else (groups - hop, groups - 1 - hop)
        pairs = [(2 * source + c, 2 * target + c) for c in range(2)]
        for k in range(chunks):
            got = swap(carried[k], "seq", pairs)
            before[k] = jnp.where(group == target, got, before[k])
            carried[k] = before[k] + total[k]
    own, other = [], []
    for k in range(chunks):
        own.append(before[k] + jnp.where(first, partner[k], 0.0))
        away = before[k] + jnp.where(first, 0.0, mine[k])
        other.append(swap(away, "seq", [(2 * g, 2 * g + 1) for g in range(groups)]))
    return own, other


def head_parts(sums):
    count = lax.axis_size("head")
    if count & (count - 1) or count > 4:
        return [lax.psum(sums, "head")]
    parts = [sums]
    for step in range(count - 1, 0, -1):
        pairs = [(i, i ^ step) for i in range(count)]
        parts.append(lax.ppermute(sums, "head", pairs))
    return parts


def per_device(queries, key_rows, values, norm_gain, cotangent):
    tokens, columns = queries.shape
    heads = columns // HEAD_DIM
    width = columns * lax.axis_size("head")
    chunks = min(CHUNKS, heads // 2)
    core = (lax.axis_index("seq") % 2).astype(jnp.int32).reshape(1)
    gain = norm_gain.reshape(1, -1)
    calls = Calls(tokens, heads, chunks, core, width)
    each = range(chunks)

    states = [calls.states(k, key_rows, values) for k in each]
    own, other = scan_chain([s[0] for s in states], [s[1] for s in states], True)
    intra = [calls.intra(k, queries, key_rows, values) for k in each]
    sums = jnp.zeros((2, tokens), f32)
    raw = []
    for k in each:
        part, sums = calls.raw(k, queries, intra[k], cotangent, gain, own[k], other[k], sums)
        raw.append(part)
    parts = head_parts(sums)
    grads = [calls.grads(k, queries, raw[k], cotangent, gain, parts) for k in each]
    after_own, after_other = scan_chain([g[1] for g in grads], [g[2] for g in grads], False)
    outs = []
    for k in each:
        normed, dq, dkp, dvp = calls.local(
            k, queries, key_rows, values, raw[k], gain, grads[k][3], grads[k][0], own[k], other[k]
        )
        dk, dv = calls.final(k, key_rows, values, dkp, dvp, after_own[k], after_other[k])
        outs.append((normed, dq, dk, dv))
    return tuple(jnp.concatenate([o[i] for o in outs], axis=1) for i in range(4))


def solution(mesh):
    in_specs = (P("seq", "head"), P("seq", "head"), P("seq", "head"), P("head"), P("seq", "head"))
    out_specs = (P("seq", "head"), P("seq", "head"), P("seq", "head"), P("seq", "head"))
    return jax.shard_map(
        per_device, mesh=mesh, in_specs=in_specs, out_specs=out_specs, check_vma=False
    )
```
